32 devices in a mesh: slab: 8 (over z, x), pencil: 4 (over y, core).
Axes of the slice: x: 2, y: 2, z: 4, core: 2. Of those that a mesh axis runs over, the one named last changes fastest.
Arguments:
- sample_tile: int32 [8192, 1], P(('slab', 'pencil')), may hold values from 0 to 31; in each aligned block of 256 rows (0 to 255, 256 to 511, ...) at most 16 rows name the same one
- sample_cell: int32 [3, 8192], P(None, ('slab', 'pencil')), may hold values from 0 to 511, as said below
- sample_frac: float32 [3, 8192], P(None, ('slab', 'pencil')), may hold values from 0 to 1
- sample_value: float32 [2, 8192], P(None, ('slab', 'pencil')), may hold values from -24 to 24
Outputs:
- volume: float32 [2, 64, 512, 512], P(None, None, 'slab', 'pencil')
The draws below stay inside these ranges and needn't reach their ends.
Inputs may be any that keep to these rules, and one draw needn't show every extreme that they name: `sample_tile`: among the 256 samples of one device no tile is named more than 16 times, and that count is reached in some device's block. `sample_cell`: row 0 is below 8, row 1 below 128, row 2 below 512.
All inputs are finite; a program needn't handle non-finite values.
Results may differ from the reference program's by a relative error of at most 0.0003.
Values sent between devices are 32-bit elements; how exact they have to be, the bound alone decides.
A program may use at most 64 MiB of HBM per device.

```python
import math
import jax
import jax.numpy as jnp
import numpy as np
from jax import lax

NY = 512
NX = 512
PLANES = 8
SAMP_DEV = 256
NZ = 64
TILES = 32
SAMPLES = 8192
CAP = 16
N_SLAB = 8
N_PENCIL = 4


def draw_sample_cell(key, part):
    sample_total = SAMP_DEV * N_SLAB * N_PENCIL
    plane_pick = jax.random.randint(jax.random.fold_in(key, 11), (sample_total,), 0, PLANES)
    row_pick = jax.random.randint(jax.random.fold_in(key, 12), (sample_total,), 0, NY // N_PENCIL)
    column_pick = jax.random.randint(jax.random.fold_in(key, 13), (sample_total,), 0, NX)
    return jnp.stack([plane_pick, row_pick, column_pick]).astype(jnp.int32)


def block_scale(key, shape, shards, low, largest):
    factor_of = 1.0
    for dim, shards_of in shards:
        draws = jax.random.uniform(jax.random.fold_in(jax.random.fold_in(key, 6), dim), (shards_of,), jnp.float32, low / len(shards), largest / len(shards))
        factor_of = factor_of * jnp.repeat(jnp.exp(draws), shape[dim] // shards_of).reshape((-1,) + (1,) * (len(shape) - 1 - dim))
    return factor_of


def deal_out(own_key, own, number, rows, number_of, top, most, skew):
    ranking = jax.random.permutation(own_key, number_of)
    crowded, usual = portions_of(number_of, rows * top, most, skew, True), portions_of(number_of, rows * top, most, skew, False)
    places = jnp.arange(number_of)

    def named(lengths, rotation):
        used = int((lengths > 0).sum())
        fixed = max(1, used // 4)
        shifted = fixed + (places - fixed + rotation * (used - fixed)) % max(1, number_of - fixed)
        return jnp.zeros((number_of,), jnp.int32).at[ranking[jnp.where(places < fixed, places, shifted)]].set(jnp.asarray(lengths, jnp.int32))

    lengths = jnp.where(number % 4 == 0, named(crowded, number // 4), named(usual, number - number // 4 - 1))
    mixed = jax.random.permutation(jax.random.fold_in(own, 3), number_of)
    source_of, receiver = mixed[0:number_of // 2 * 2:2], mixed[1:number_of // 2 * 2:2]
    room = jnp.minimum(lengths[source_of] - 1, most - lengths[receiver]) // 2
    room = jnp.where((source_of == ranking[0]) | (receiver == ranking[0]) | (lengths[receiver] == 0), 0, jnp.maximum(room, 0))
    shifted = jax.random.randint(jax.random.fold_in(own, 4), (number_of // 2,), 0, 1 << 20) % (room + 1)
    lengths = lengths.at[source_of].add(-shifted).at[receiver].add(shifted)
    items = jnp.searchsorted(jnp.cumsum(lengths), jnp.arange(rows * top), side="right").astype(jnp.int32)
    listing = items.reshape(top, rows).T
    listing = listing[jax.random.permutation(jax.random.fold_in(own, 1), rows)]
    rotation = jax.random.randint(jax.random.fold_in(own, 2), (rows, 1), 0, top)
    return jnp.take_along_axis(listing, (jnp.arange(top)[None, :] + rotation) % top, axis=1)


def portions_of(amount, total, bound, skew, full):
    loads = [(1 << 20) // math.isqrt(grade ** skew) + 1 for grade in range(1, amount + 1)]
    largest = bound if full else min(bound, max(-(-total // amount), total * loads[0] // sum(loads)))
    least = 1 if total - largest >= amount - 1 else 0
    holding, rest = [largest] + [least] * (amount - 1), total - largest - least * (amount - 1)
    while rest > 0:
        candidates = [i for i in range(1, amount) if holding[i] < largest] or [i for i in range(1, amount) if holding[i] < bound]
        mass, left = sum([loads[i] for i in candidates]), rest
        for i in candidates:
            more = min(bound - holding[i], max(1, left * loads[i] // mass), rest)
            holding[i] = holding[i] + more
            rest = rest - more
    return np.array(holding)


def gaussian(rng, dims, spread, reach, cuts=(), kind=jnp.bfloat16):
    gain = block_scale(rng, dims, cuts, -0.22, 0.18) if cuts else 1.0
    entries = jax.random.normal(rng, dims, jnp.float32) * spread * gain
    return jnp.minimum(jnp.maximum(entries, -reach), reach).astype(kind)


def setup_inputs(seed: int = 0) -> dict:
    streams_of = jax.random.split(jax.random.key(seed), 5)
    sample_tile_keys = jax.random.split(jax.random.fold_in(streams_of[0], 1), SAMPLES // SAMP_DEV)
    sample_tile_turns = jax.random.permutation(jax.random.fold_in(streams_of[0], 3), SAMPLES // SAMP_DEV)
    sample_tile = jax.vmap(lambda own, number: deal_out(jax.random.fold_in(streams_of[0], 2), own, number, SAMP_DEV, TILES, 1, CAP, 2))(sample_tile_keys, sample_tile_turns).reshape((SAMPLES, 1))
    sample_cell = draw_sample_cell(jax.random.fold_in(streams_of[4], 71), 0)
    sample_frac = jnp.clip(1.0 * jax.random.uniform(streams_of[2], (3, SAMPLES), jnp.float32) ** block_scale(streams_of[2], (3, SAMPLES), ((1, 32),), -0.2, 0.2), 0.0, 1.0)
    sample_value = gaussian(streams_of[3], (2, SAMPLES), 4.0, 24.0, ((1, 32),), jnp.float32)
    return {"sample_tile": sample_tile, "sample_cell": sample_cell, "sample_frac": sample_frac, "sample_value": sample_value}


beta_shape = 18.64

def bessel_zero(value):
    quarter = value * value * 0.25
    term = jnp.ones_like(value)
    total = jnp.ones_like(value)
    for order in range(1, 41):
        term = term * quarter / float(order * order)
        total = total + term
    return total

def kernel_weights(offset):
    tap_offsets = jnp.arange(8, dtype=jnp.float32) - 3.0
    scaled_gap = (tap_offsets[None, :] - offset[:, None]) * 0.25
    radicand = jnp.maximum(1.0 - scaled_gap * scaled_gap, 0.0)
    numerator = bessel_zero(beta_shape * jnp.sqrt(radicand))
    return numerator / bessel_zero(jnp.full((), beta_shape, jnp.float32))

def reference(sample_tile, sample_cell, sample_frac, sample_value):
    owner_tile = sample_tile[:, 0]
    row_count = NY // N_PENCIL
    base_z = owner_tile // N_PENCIL * PLANES + sample_cell[0]
    base_y = owner_tile % N_PENCIL * row_count + sample_cell[1]
    base_x = sample_cell[2]
    total_count = owner_tile.shape[0]
    block_size = math.gcd(total_count, 8192)
    block_total = total_count // block_size
    tap_offsets = jnp.arange(8, dtype=jnp.int32)

    def add_block(carry, pieces):
        real_flat, imag_flat = carry
        piece_z, piece_y, piece_x, piece_frac, piece_value = pieces
        weight_z = kernel_weights(piece_frac[0])
        weight_y = kernel_weights(piece_frac[1])
        weight_x = kernel_weights(piece_frac[2])
        plane_at = (piece_z[:, None] + tap_offsets[None, :]) % NZ
        row_at = (piece_y[:, None] + tap_offsets[None, :]) % NY
        column_at = (piece_x[:, None] + tap_offsets[None, :]) % NX
        target = ((plane_at[:, :, None, None] * NY + row_at[:, None, :, None]) * NX + column_at[:, None, None, :]).reshape(block_size, 512)
        weight = (weight_z[:, :, None, None] * weight_y[:, None, :, None] * weight_x[:, None, None, :]).reshape(block_size, 512)
        real_flat = real_flat.at[target].add(weight * piece_value[0][:, None])
        imag_flat = imag_flat.at[target].add(weight * piece_value[1][:, None])
        return ((real_flat, imag_flat), None)
    stacked = (base_z.reshape(block_total, block_size), base_y.reshape(block_total, block_size), base_x.reshape(block_total, block_size), sample_frac.reshape(3, block_total, block_size).transpose(1, 0, 2), sample_value.reshape(2, block_total, block_size).transpose(1, 0, 2))
    start_grid = (jnp.zeros((NZ * NY * NX,), jnp.float32), jnp.zeros((NZ * NY * NX,), jnp.float32))
    (real_flat, imag_flat), _ = lax.scan(add_block, start_grid, stacked)
    field_grid = lax.complex(real_flat.reshape(NZ, NY, NX), imag_flat.reshape(NZ, NY, NX))
    result = jnp.fft.ifftn(field_grid, norm='ortho')
    return jnp.stack([jnp.real(result), jnp.imag(result)]).astype(jnp.float32)
```

```python
import functools
import math

import jax
import jax.numpy as jnp
import numpy as np
from jax import lax
from jax.experimental import pallas as pl
from jax.experimental.pallas import tpu as pltpu
from jax.sharding import PartitionSpec as P

NY = 512
NX = 512
PLANES = 8
TAPS = 8
WINDOW = PLANES + TAPS - 1
LOW = 16
CHUNK = 128
BETA = 18.64
F32 = jnp.float32
BF16 = jnp.bfloat16


def series():
    quarter = BETA * BETA / 4.0
    terms = [1.0]
    for order in range(1, 41):
        terms.append(terms[-1] * quarter / float(order * order))
    total = sum(terms)
    return [term / total for term in terms]


SERIES = series()


def tap_weights(frac, taps):
    gap = (taps - 3.0 - frac) * 0.25
    radicand = jnp.maximum(1.0 - gap * gap, 0.0)
    total = jnp.full(radicand.shape, SERIES[-1], F32)
    for coefficient in SERIES[-2::-1]:
        total = total * radicand + coefficient
    return total


def placed(weights, anchor, rows):
    gap = lax.broadcasted_iota(jnp.int32, (rows, anchor.shape[1]), 0) - anchor
    total = jnp.where(gap == 0, weights[0:1], 0.0)
    for tap in range(1, TAPS):
        total = jnp.where(gap == tap, weights[tap : tap + 1], total)
    return total


def halves(value):
    high = value.astype(BF16)
    return high, (value - high.astype(F32)).astype(BF16)


def fine_dot(left, right):
    left_high, left_low = left
    right_high, right_low = halves(right)
    dot = functools.partial(jnp.dot, preferred_element_type=F32)
    return dot(left_high, right_high) + (dot(left_high, right_low) + dot(left_low, right_high))


def kernel(
    n_src, n_slab, per, room, ny, nz,
    starts, feats, tap_y, phase_y, tap_x, phase_x, table_z, out, rows, packed, grid_re, grid_im, left,
):
    slab_here = lax.axis_index("slab")
    pencil_here = lax.axis_index("pencil")
    nx = out.shape[2]

    @pl.loop(0, n_src)
    def _(src):
        rows[pl.ds(pl.multiple_of(src * per, per), per), 0:8] = feats[src].T

    grid_re[...] = jnp.zeros_like(grid_re)
    grid_im[...] = jnp.zeros_like(grid_im)
    taps = lax.broadcasted_iota(jnp.int32, (TAPS, CHUNK), 0).astype(F32)
    lanes = lax.broadcasted_iota(jnp.int32, (8, CHUNK), 1)
    ty, hy = halves(tap_y[slab_here]), halves(phase_y[slab_here])
    tx, hx = halves(tap_x[pencil_here]), halves(phase_x[pencil_here])

    @pl.loop(0, n_slab)
    def _(slab):
        def pack(src, filled):
            first = starts[src, slab]
            packed[pl.ds(filled, room), :] = rows[pl.ds(src * per + first, room), :]
            return filled + starts[src, slab + 1] - first

        filled = lax.fori_loop(0, n_src, pack, jnp.int32(0))

        @pl.loop(0, (filled + CHUNK - 1) // CHUNK)
        def _(chunk):
            base = pl.multiple_of(chunk * CHUNK, CHUNK)
            f = packed[pl.ds(base, CHUNK), :].T[0:8]
            f = jnp.where(lanes + base < filled, f, 0.0)
            whole = f[0:3].astype(jnp.int32)
            depth = whole[0:1] - slab * PLANES
            high_y, high_x = whole[1:2] // LOW, whole[2:3] // LOW
            low_y, low_x = whole[1:2] - high_y * LOW, whole[2:3] - high_x * LOW
            weight_z = placed(tap_weights(f[3:4], taps), depth, 2 * PLANES)
            place_y = placed(tap_weights(f[4:5], taps), low_y, 2 * LOW)
            place_x = placed(tap_weights(f[5:6], taps), low_x, 2 * LOW)
            counter = lax.broadcasted_iota(jnp.int32, (NY // LOW, CHUNK), 0)
            hit_y = counter == high_y
            hit_x = (counter == high_x).astype(F32)
            value_y = jnp.concatenate([jnp.where(hit_y, f[6:7], 0.0), jnp.where(hit_y, f[7:8], 0.0)], axis=0)
            near, far = fine_dot(ty, place_y), fine_dot(hy, value_y)
            b_re = near[:ny] * far[:ny] - near[ny:] * far[ny:]
            b_im = near[:ny] * far[ny:] + near[ny:] * far[:ny]
            near, far = fine_dot(tx, place_x), fine_dot(hx, hit_x)
            c_re = near[:nx] * far[:nx] - near[nx:] * far[nx:]
            c_im = near[:nx] * far[nx:] + near[nx:] * far[:nx]
            right = jnp.concatenate(
                [jnp.concatenate([c_re, -c_im], axis=1), jnp.concatenate([c_im, c_re], axis=1)], axis=0
            )
            right_high, right_low = halves(right)
            both = jnp.concatenate([b_re, b_im], axis=1)
            for z in range(WINDOW):
                line = weight_z[z : z + 1]
                high, low = halves(both * jnp.concatenate([line, line], axis=1))
                left[z * ny : (z + 1) * ny, 0 : 2 * CHUNK] = high
                left[z * ny : (z + 1) * ny, 2 * CHUNK : 4 * CHUNK] = low
                left[z * ny : (z + 1) * ny, 4 * CHUNK : 6 * CHUNK] = high
            right_all = jnp.concatenate([right_high, right_high, right_low], axis=1)
            sums = lax.dot_general(
                left[...], right_all, (((1,), (1,)), ((), ())), preferred_element_type=F32
            )
            at = pl.ds(pl.multiple_of(slab * (PLANES * ny), PLANES * ny), WINDOW * ny)
            grid_re[at, :] += sums[:, :nx]
            grid_im[at, :] += sums[:, nx:]

    depth_all = table_z.shape[1]
    tz = halves(table_z[...])

    @pl.loop(0, ny)
    def _(row):
        pick = pl.ds(row, depth_all, stride=ny)
        sums = fine_dot(tz, jnp.concatenate([grid_re[pick, :], grid_im[pick, :]], axis=1))
        place = pl.ds(row, nz, stride=ny)
        out[0, place, :] = sums[:nz, :nx] - sums[nz:, nx:]
        out[1, place, :] = sums[nz:, :nx] + sums[:nz, nx:]


def turns(outer, inner, length):
    angle = 2.0 * np.pi * ((outer * inner) % length) / length
    return np.cos(angle), np.sin(angle)


def tables(n_slab, n_pencil, nz):
    ny, nx = NY // n_slab, NX // n_pencil
    near, far = np.arange(2 * LOW), np.arange(NY // LOW) * LOW

    def stacked(count, width, inner, length):
        outer = np.arange(count * width).reshape(count, width, 1)
        return turns(outer, inner, length)

    cy, sy = stacked(n_slab, ny, near, NY)
    tap_y = np.concatenate([cy, sy], axis=1)
    cy, sy = stacked(n_slab, ny, far, NY)
    phase_y = np.concatenate(
        [np.concatenate([cy, -sy], axis=2), np.concatenate([sy, cy], axis=2)], axis=1
    )
    cx, sx = stacked(n_pencil, nx, near, NX)
    tap_x = np.concatenate([cx, sx], axis=1)
    cx, sx = stacked(n_pencil, nx, far, NX)
    phase_x = np.concatenate([cx, sx], axis=1)
    cz, sz = turns(np.arange(nz)[:, None], np.arange(nz + PLANES)[None, :], nz)
    table_z = np.concatenate([cz, sz], axis=0) / math.sqrt(nz * NY * NX)
    return [x.astype(np.float32) for x in (tap_y, phase_y, tap_x, phase_x, table_z)]


def shards(n_slab, n_pencil, sample_tile, sample_cell, sample_frac, sample_value):
    n_src = n_slab * n_pencil
    per = sample_tile.shape[0]
    nz = PLANES * n_slab
    ny, nx = NY // n_slab, NX // n_pencil
    capacity = max(2, 2 * per // n_src)
    room = -(-n_pencil * capacity // 8) * 8
    owner = sample_tile[:, 0]
    base_z = owner // n_pencil * PLANES + sample_cell[0]
    base_y = owner % n_pencil * (NY // n_pencil) + sample_cell[1]
    anchor = jnp.stack([base_z, base_y, sample_cell[2]]).astype(F32)
    mine = jnp.concatenate([anchor, sample_frac, sample_value], axis=0)
    order = jnp.arange(per, dtype=jnp.int32)
    key = base_z * per + order
    rank = jnp.sum((key[None, :] < key[:, None]).astype(jnp.int32), axis=1)
    shuffle = (rank[:, None] == order[None, :]).astype(F32)
    mine = jnp.dot(mine, shuffle, precision=lax.Precision.HIGHEST, preferred_element_type=F32)
    feats = lax.all_gather(mine, ("slab", "pencil"), axis=0, tiled=False)
    slab_of = feats[:, 0, :].astype(jnp.int32) // PLANES
    bins = jnp.arange(n_slab + 1, dtype=jnp.int32)
    starts = jnp.sum((slab_of[:, None, :] < bins[None, :, None]).astype(jnp.int32), axis=2)
    most = n_src * room
    vmem = pl.BlockSpec(memory_space=pltpu.VMEM)
    volume = pl.pallas_call(
        functools.partial(kernel, n_src, n_slab, per, room, ny, nz),
        out_shape=jax.ShapeDtypeStruct((2, nz * ny, nx), F32),
        in_specs=[pl.BlockSpec(memory_space=pltpu.SMEM)] + [vmem] * 6,
        out_specs=vmem,
        scratch_shapes=[
            pltpu.VMEM((n_src * per + room, 128), F32),
            pltpu.VMEM((most + room, 128), F32),
            pltpu.VMEM(((nz + PLANES) * ny, nx), F32),
            pltpu.VMEM(((nz + PLANES) * ny, nx), F32),
            pltpu.VMEM((WINDOW * ny, 6 * CHUNK), BF16),
        ],
        compiler_params=pltpu.CompilerParams(vmem_limit_bytes=62 * 1024 * 1024),
        name="volume",
    )(starts, feats, *tables(n_slab, n_pencil, nz))
    return volume.reshape(2, nz, ny, nx)


def solution(mesh):
    placed_as = (
        P(("slab", "pencil"), None),
        P(None, ("slab", "pencil")),
        P(None, ("slab", "pencil")),
        P(None, ("slab", "pencil")),
    )
    return jax.shard_map(
        functools.partial(shards, mesh.shape["slab"], mesh.shape["pencil"]),
        mesh=mesh,
        in_specs=placed_as,
        out_specs=P(None, None, "slab", "pencil"),
        check_vma=False,
    )
```

```python
import functools
import math

import jax
import jax.numpy as jnp
import numpy as np
from jax import lax
from jax.experimental import pallas as pl
from jax.experimental.pallas import tpu as pltpu
from jax.sharding import PartitionSpec as P

NY = 512
NX = 512
PLANES = 8
TAPS = 8
WINDOW = PLANES + TAPS - 1
LOW = 16
CHUNK = 128
GROUP = 256
BETA = 18.64
F32 = jnp.float32
BF16 = jnp.bfloat16


def series():
    quarter = BETA * BETA / 4.0
    terms = [1.0]
    for order in range(1, 41):
        terms.append(terms[-1] * quarter / float(order * order))
    total = sum(terms)
    return [term / total for term in terms]


SERIES = series()


def tap_weights(frac, taps):
    gap = (taps - 3.0 - frac) * 0.25
    radicand = jnp.maximum(1.0 - gap * gap, 0.0)
    total = jnp.full(radicand.shape, SERIES[-1], F32)
    for coefficient in SERIES[-2::-1]:
        total = total * radicand + coefficient
    return total


def placed(weights, anchor, rows):
    gap = lax.broadcasted_iota(jnp.int32, (rows, anchor.shape[1]), 0) - anchor
    total = jnp.where(gap == 0, weights[0:1], 0.0)
    for tap in range(1, TAPS):
        total = jnp.where(gap == tap, weights[tap : tap + 1], total)
    return total


def halves(value):
    high = value.astype(BF16)
    return high, (value - high.astype(F32)).astype(BF16)


def stack_left(value):
    high = value.astype(jnp.bfloat16)
    low = (value - high.astype(np.float32)).astype(jnp.bfloat16)
    return np.concatenate([high, high, low], axis=-1)


def fine_dot(left, right):
    high, low = halves(right)
    return jnp.dot(left, jnp.concatenate([high, low, high], axis=0), preferred_element_type=F32)


def gather_kernel(n_slab, n_pencil, mine, out, send_sem, recv_sem, own_sem):
    count = n_slab * n_pencil
    me = lax.axis_index("slab") * n_pencil + lax.axis_index("pencil")

    def name(step):
        target = lax.rem(me + step, count)
        return {"slab": target // n_pencil, "pencil": lax.rem(target, n_pencil)}

    own = pltpu.make_async_copy(mine, out.at[me], own_sem)
    own.start()
    barrier = pltpu.get_barrier_semaphore()

    @pl.loop(1, count)
    def _(step):
        pl.semaphore_signal(barrier, inc=1, device_id=name(step), device_id_type=pl.DeviceIdType.MESH)

    pl.semaphore_wait(barrier, count - 1)

    def send(step, slot):
        return pltpu.make_async_remote_copy(
            src_ref=mine,
            dst_ref=out.at[slot],
            send_sem=send_sem.at[step - 1],
            recv_sem=recv_sem.at[step - 1],
            device_id=name(step),
            device_id_type=pl.DeviceIdType.MESH,
        )

    @pl.loop(1, count)
    def _(step):
        send(step, me).start()

    own.wait()

    @pl.loop(1, count)
    def _(step):
        send(step, lax.rem(me + count - step, count)).wait_recv()

    @pl.loop(1, count)
    def _(step):
        send(step, me).wait_send()


def gather_all(n_slab, n_pencil, mine):
    count = n_slab * n_pencil
    vmem = pl.BlockSpec(memory_space=pltpu.VMEM)
    return pl.pallas_call(
        functools.partial(gather_kernel, n_slab, n_pencil),
        out_shape=jax.ShapeDtypeStruct((count,) + mine.shape, mine.dtype),
        in_specs=[vmem],
        out_specs=vmem,
        scratch_shapes=[
            pltpu.SemaphoreType.DMA((count - 1,)),
            pltpu.SemaphoreType.DMA((count - 1,)),
            pltpu.SemaphoreType.DMA,
        ],
        compiler_params=pltpu.CompilerParams(collective_id=0, has_side_effects=True),
        name="gather_samples",
    )(mine)


def kernel(
    n_src, n_slab, per, room, ny, nz,
    starts, feats, tap_y, phase_y, tap_x, phase_x, table_z, out,
    rows, packed, grid_re, grid_im, left, both, right, depths,
):
    slab_here = lax.axis_index("slab")
    pencil_here = lax.axis_index("pencil")
    nx = out.shape[2]
    taps = lax.broadcasted_iota(jnp.int32, (TAPS, per), 0).astype(F32)

    @pl.loop(0, n_src, unroll=2)
    def _(src):
        f = feats[src]
        pieces = [f] + [tap_weights(f[3 + d : 4 + d], taps) for d in range(3)]
        rows[pl.ds(pl.multiple_of(src * per, per), per), 0:32] = jnp.concatenate(pieces, axis=0).T

    grid_re[...] = jnp.zeros_like(grid_re)
    grid_im[...] = jnp.zeros_like(grid_im)
    lanes = lax.broadcasted_iota(jnp.int32, (32, GROUP), 1)
    counter = lax.broadcasted_iota(jnp.int32, (NY // LOW, GROUP), 0)
    ty, hy = tap_y[slab_here], phase_y[slab_here]
    tx, hx = tap_x[pencil_here], phase_x[pencil_here]

    @pl.loop(0, n_slab)
    def _(slab):
        def pack(src, filled):
            first = starts[src, slab]
            packed[pl.ds(filled, room), :] = rows[pl.ds(src * per + first, room), :]
            return filled + starts[src, slab + 1] - first

        filled = lax.fori_loop(0, n_src, pack, jnp.int32(0), unroll=4)

        @pl.loop(0, (filled + GROUP - 1) // GROUP)
        def _(group):
            base = pl.multiple_of(group * GROUP, GROUP)
            f = packed[pl.ds(base, GROUP), :].T[0:32]
            f = jnp.where(lanes + base < filled, f, 0.0)
            whole = f[0:3].astype(jnp.int32)
            high_y, high_x = whole[1:2] // LOW, whole[2:3] // LOW
            weight_z = placed(f[8:16], whole[0:1] - slab * PLANES, 2 * PLANES)
            place_y = placed(f[16:24], whole[1:2] - high_y * LOW, 2 * LOW)
            place_x = placed(f[24:32], whole[2:3] - high_x * LOW, 2 * LOW)
            hit_y = counter == high_y
            hit_x = (counter == high_x).astype(F32).astype(BF16)
            value_y = jnp.concatenate([jnp.where(hit_y, f[6:7], 0.0), jnp.where(hit_y, f[7:8], 0.0)], axis=0)
            near, far = fine_dot(ty, place_y), fine_dot(hy, value_y)
            b_re = near[:ny] * far[:ny] - near[ny:] * far[ny:]
            b_im = near[:ny] * far[ny:] + near[ny:] * far[:ny]
            near = fine_dot(tx, place_x)
            far = jnp.dot(hx, jnp.concatenate([hit_x, hit_x], axis=0), preferred_element_type=F32)
            c_re = near[:nx] * far[:nx] - near[nx:] * far[nx:]
            c_im = near[:nx] * far[nx:] + near[nx:] * far[:nx]
            re_high, re_low = halves(c_re)
            im_high, im_low = halves(c_im)
            for part in range(GROUP // CHUNK):
                cut = slice(part * CHUNK, (part + 1) * CHUNK)
                chunk = group * (GROUP // CHUNK) + part
                depths[chunk] = weight_z[:, cut]
                both[chunk, :, :CHUNK] = b_re[:, cut]
                both[chunk, :, CHUNK:] = b_im[:, cut]
                for at, (re, im) in enumerate(((re_high, im_high), (re_high, im_high), (re_low, im_low))):
                    first, second = at * 2 * CHUNK, (at * 2 + 1) * CHUNK
                    right[chunk, :nx, first : first + CHUNK] = re[:, cut]
                    right[chunk, :nx, second : second + CHUNK] = -im[:, cut]
                    right[chunk, nx:, first : first + CHUNK] = im[:, cut]
                    right[chunk, nx:, second : second + CHUNK] = re[:, cut]

        @pl.loop(0, (filled + CHUNK - 1) // CHUNK)
        def _(chunk):
            for z in range(WINDOW):
                line = depths[chunk, z : z + 1, :]
                high, low = halves(both[chunk] * jnp.concatenate([line, line], axis=1))
                left[z * ny : (z + 1) * ny, 0 : 2 * CHUNK] = high
                left[z * ny : (z + 1) * ny, 2 * CHUNK : 4 * CHUNK] = low
                left[z * ny : (z + 1) * ny, 4 * CHUNK : 6 * CHUNK] = high
            sums = lax.dot_general(
                left[...], right[chunk], (((1,), (1,)), ((), ())), preferred_element_type=F32
            )
            at = pl.ds(pl.multiple_of(slab * (PLANES * ny), PLANES * ny), WINDOW * ny)
            grid_re[at, :] += sums[:, :nx]
            grid_im[at, :] += sums[:, nx:]

    tz = table_z[...]
    depth_all = table_z.shape[1] // 3

    @pl.loop(0, ny, unroll=4)
    def _(row):
        pick = pl.ds(row, depth_all, stride=ny)
        sums = fine_dot(tz, jnp.concatenate([grid_re[pick, :], grid_im[pick, :]], axis=1))
        place = pl.ds(row, nz, stride=ny)
        out[0, place, :] = sums[:nz, :nx] - sums[nz:, nx:]
        out[1, place, :] = sums[nz:, :nx] + sums[:nz, nx:]


def turns(outer, inner, length):
    angle = 2.0 * np.pi * ((outer * inner) % length) / length
    return np.cos(angle), np.sin(angle)


def tables(n_slab, n_pencil, nz):
    ny, nx = NY // n_slab, NX // n_pencil
    near, far = np.arange(2 * LOW), np.arange(NY // LOW) * LOW

    def stacked(count, width, inner, length):
        outer = np.arange(count * width).reshape(count, width, 1)
        return turns(outer, inner, length)

    cy, sy = stacked(n_slab, ny, near, NY)
    tap_y = np.concatenate([cy, sy], axis=1)
    cy, sy = stacked(n_slab, ny, far, NY)
    phase_y = np.concatenate(
        [np.concatenate([cy, -sy], axis=2), np.concatenate([sy, cy], axis=2)], axis=1
    )
    cx, sx = stacked(n_pencil, nx, near, NX)
    tap_x = np.concatenate([cx, sx], axis=1)
    cx, sx = stacked(n_pencil, nx, far, NX)
    phase_x = np.concatenate([cx, sx], axis=1)
    cz, sz = turns(np.arange(nz)[:, None], np.arange(nz + 2 * PLANES)[None, :], nz)
    table_z = np.concatenate([cz, sz], axis=0) / math.sqrt(nz * NY * NX)
    stacks = [stack_left(x.astype(np.float32)) for x in (tap_y, phase_y, tap_x, table_z)]
    exact_right = np.delete(stack_left(phase_x.astype(np.float32)), np.s_[: NY // LOW], axis=-1)
    return stacks[0], stacks[1], stacks[2], exact_right, stacks[3]


def shards(n_slab, n_pencil, sample_tile, sample_cell, sample_frac, sample_value):
    n_src = n_slab * n_pencil
    per = sample_tile.shape[0]
    nz = PLANES * n_slab
    ny, nx = NY // n_slab, NX // n_pencil
    capacity = max(2, 2 * per // n_src)
    room = -(-n_pencil * capacity // 8) * 8
    owner = sample_tile[:, 0]
    base_z = owner // n_pencil * PLANES + sample_cell[0]
    base_y = owner % n_pencil * (NY // n_pencil) + sample_cell[1]
    anchor = jnp.stack([base_z, base_y, sample_cell[2]]).astype(F32)
    mine = jnp.concatenate([anchor, sample_frac, sample_value], axis=0)
    order = jnp.arange(per, dtype=jnp.int32)
    key = base_z * per + order
    rank = jnp.sum((key[None, :] < key[:, None]).astype(jnp.int32), axis=1)
    shuffle = (rank[:, None] == order[None, :]).astype(F32)
    mine = jnp.dot(mine, shuffle, precision=lax.Precision.HIGHEST, preferred_element_type=F32)
    feats = gather_all(n_slab, n_pencil, mine)
    slab_of = feats[:, 0, :].astype(jnp.int32) // PLANES
    bins = jnp.arange(n_slab + 1, dtype=jnp.int32)
    starts = jnp.sum((slab_of[:, None, :] < bins[None, :, None]).astype(jnp.int32), axis=2)
    most = n_src * room
    chunks = -(-most // GROUP) * (GROUP // CHUNK)
    vmem = pl.BlockSpec(memory_space=pltpu.VMEM)
    volume = pl.pallas_call(
        functools.partial(kernel, n_src, n_slab, per, room, ny, nz),
        out_shape=jax.ShapeDtypeStruct((2, nz * ny, nx), F32),
        in_specs=[pl.BlockSpec(memory_space=pltpu.SMEM)] + [vmem] * 6,
        out_specs=vmem,
        scratch_shapes=[
            pltpu.VMEM((n_src * per + room, 128), F32),
            pltpu.VMEM((-(-most // GROUP) * GROUP + room, 128), F32),
            pltpu.VMEM(((nz + 2 * PLANES) * ny, nx), F32),
            pltpu.VMEM(((nz + 2 * PLANES) * ny, nx), F32),
            pltpu.VMEM((WINDOW * ny, 6 * CHUNK), BF16),
            pltpu.VMEM((chunks, ny, 2 * CHUNK), F32),
            pltpu.VMEM((chunks, 2 * nx, 6 * CHUNK), BF16),
            pltpu.VMEM((chunks, 2 * PLANES, CHUNK), F32),
        ],
        compiler_params=pltpu.CompilerParams(vmem_limit_bytes=67043328),
        name="volume",
    )(starts, feats, *tables(n_slab, n_pencil, nz))
    return volume.reshape(2, nz, ny, nx)


def solution(mesh):
    placed_as = (
        P(("slab", "pencil"), None),
        P(None, ("slab", "pencil")),
        P(None, ("slab", "pencil")),
        P(None, ("slab", "pencil")),
    )
    return jax.shard_map(
        functools.partial(shards, mesh.shape["slab"], mesh.shape["pencil"]),
        mesh=mesh,
        in_specs=placed_as,
        out_specs=P(None, None, "slab", "pencil"),
        check_vma=False,
    )
```

```python
import functools
import math

import jax
import jax.numpy as jnp
import numpy as np
from jax import lax
from jax.experimental import pallas as pl
from jax.experimental.pallas import tpu as pltpu
from jax.sharding import PartitionSpec as P

NY = 512
NX = 512
PLANES = 8
TAPS = 8
WINDOW = PLANES + TAPS - 1
LOW = 16
CHUNK = 128
GROUP = 256
BINS = 4
BETA = 18.64
F32 = jnp.float32
BF16 = jnp.bfloat16


def series():
    quarter = BETA * BETA / 4.0
    terms = [1.0]
    for order in range(1, 41):
        terms.append(terms[-1] * quarter / float(order * order))
    total = sum(terms)
    return [term / total for term in terms]


SERIES = series()


def tap_weights(frac, taps):
    gap = (taps - 3.0 - frac) * 0.25
    radicand = jnp.maximum(1.0 - gap * gap, 0.0)
    total = jnp.full(radicand.shape, SERIES[-1], F32)
    for coefficient in SERIES[-2::-1]:
        total = total * radicand + coefficient
    return total


def placed(weights, anchor, rows):
    gap = lax.broadcasted_iota(jnp.int32, (rows, anchor.shape[1]), 0) - anchor
    total = jnp.where(gap == 0, weights[0:1], 0.0)
    for tap in range(1, TAPS):
        total = jnp.where(gap == tap, weights[tap : tap + 1], total)
    return total


def halves(value):
    high = value.astype(BF16)
    return high, (value - high.astype(F32)).astype(BF16)


def stack_left(value):
    high = value.astype(jnp.bfloat16)
    low = (value - high.astype(np.float32)).astype(jnp.bfloat16)
    return np.concatenate([high, high, low], axis=-1)


def fine_dot(left, right):
    high, low = halves(right)
    return jnp.dot(left, jnp.concatenate([high, low, high], axis=0), preferred_element_type=F32)


def gather_kernel(n_slab, n_pencil, mine, out, send_sem, recv_sem, own_sem):
    count = n_slab * n_pencil
    me = lax.axis_index("slab") * n_pencil + lax.axis_index("pencil")

    def name(step):
        target = lax.rem(me + step, count)
        return {"slab": target // n_pencil, "pencil": lax.rem(target, n_pencil)}

    own = pltpu.make_async_copy(mine, out.at[me], own_sem)
    own.start()
    barrier = pltpu.get_barrier_semaphore()

    @pl.loop(1, count)
    def _(step):
        pl.semaphore_signal(barrier, inc=1, device_id=name(step), device_id_type=pl.DeviceIdType.MESH)

    pl.semaphore_wait(barrier, count - 1)

    def send(step, slot):
        return pltpu.make_async_remote_copy(
            src_ref=mine,
            dst_ref=out.at[slot],
            send_sem=send_sem.at[step - 1],
            recv_sem=recv_sem.at[step - 1],
            device_id=name(step),
            device_id_type=pl.DeviceIdType.MESH,
        )

    @pl.loop(1, count)
    def _(step):
        send(step, me).start()

    own.wait()

    @pl.loop(1, count)
    def _(step):
        send(step, lax.rem(me + count - step, count)).wait_recv()

    @pl.loop(1, count)
    def _(step):
        send(step, me).wait_send()


def gather_all(n_slab, n_pencil, mine):
    count = n_slab * n_pencil
    vmem = pl.BlockSpec(memory_space=pltpu.VMEM)
    return pl.pallas_call(
        functools.partial(gather_kernel, n_slab, n_pencil),
        out_shape=jax.ShapeDtypeStruct((count,) + mine.shape, mine.dtype),
        in_specs=[vmem],
        out_specs=vmem,
        scratch_shapes=[
            pltpu.SemaphoreType.DMA((count - 1,)),
            pltpu.SemaphoreType.DMA((count - 1,)),
            pltpu.SemaphoreType.DMA,
        ],
        compiler_params=pltpu.CompilerParams(collective_id=0, has_side_effects=True),
        name="gather_samples",
    )(mine)


def kernel(
    n_src, n_slab, per, room, ny, nz,
    starts, feats, tap_y, phase_y, tap_x, phase_x, table_z, out,
    rows, packed, grid_re, grid_im, left, both, right, depths,
):
    slab_here = lax.axis_index("slab")
    pencil_here = lax.axis_index("pencil")
    nx = out.shape[3]
    short = min(room, 16)
    taps = lax.broadcasted_iota(jnp.int32, (TAPS, per), 0).astype(F32)

    @pl.loop(0, n_src, unroll=2)
    def _(src):
        f = feats[src]
        pieces = [f] + [tap_weights(f[3 + d : 4 + d], taps) for d in range(3)]
        rows[pl.ds(pl.multiple_of(src * per, per), per), 0:32] = jnp.concatenate(pieces, axis=0).T

    grid_re[...] = jnp.zeros_like(grid_re)
    grid_im[...] = jnp.zeros_like(grid_im)
    lanes = lax.broadcasted_iota(jnp.int32, (32, GROUP), 1)
    counter = lax.broadcasted_iota(jnp.int32, (NY // LOW, GROUP), 0)
    ty, hy = tap_y[slab_here], phase_y[slab_here]
    tx, hx = tap_x[pencil_here], phase_x[pencil_here]

    @pl.loop(0, n_slab)
    def _(slab):
        ends = []
        filled = jnp.int32(0)
        for part in range(BINS):

            def pack(src, filled, part=part):
                first = starts[src, slab * BINS + part]
                count = starts[src, slab * BINS + part + 1] - first
                packed[pl.ds(filled, short), :] = rows[pl.ds(src * per + first, short), :]
                if short < room:

                    @pl.when(count > short)
                    def _():
                        rest = room - short
                        packed[pl.ds(filled + short, rest), :] = rows[pl.ds(src * per + first + short, rest), :]

                return filled + count

            filled = lax.fori_loop(0, n_src, pack, filled, unroll=4)
            ends.append(filled)

        @pl.loop(0, (filled + GROUP - 1) // GROUP)
        def _(group):
            base = pl.multiple_of(group * GROUP, GROUP)
            f = packed[pl.ds(base, GROUP), :].T[0:32]
            f = jnp.where(lanes + base < filled, f, 0.0)
            whole = f[0:3].astype(jnp.int32)
            high_y, high_x = whole[1:2] // LOW, whole[2:3] // LOW
            weight_z = placed(f[8:16], whole[0:1] - slab * PLANES, 2 * PLANES)
            place_y = placed(f[16:24], whole[1:2] - high_y * LOW, 2 * LOW)
            place_x = placed(f[24:32], whole[2:3] - high_x * LOW, 2 * LOW)
            hit_y = counter == high_y
            hit_x = (counter == high_x).astype(F32).astype(BF16)
            value_y = jnp.concatenate([jnp.where(hit_y, f[6:7], 0.0), jnp.where(hit_y, f[7:8], 0.0)], axis=0)
            near, far = fine_dot(ty, place_y), fine_dot(hy, value_y)
            b_re = near[:ny] * far[:ny] - near[ny:] * far[ny:]
            b_im = near[:ny] * far[ny:] + near[ny:] * far[:ny]
            near = fine_dot(tx, place_x)
            far = jnp.dot(hx, jnp.concatenate([hit_x, hit_x], axis=0), preferred_element_type=F32)
            c_re = near[:nx] * far[:nx] - near[nx:] * far[nx:]
            c_im = near[:nx] * far[nx:] + near[nx:] * far[:nx]
            re_high, re_low = halves(c_re)
            im_high, im_low = halves(c_im)
            for part in range(GROUP // CHUNK):
                cut = slice(part * CHUNK, (part + 1) * CHUNK)
                chunk = group * (GROUP // CHUNK) + part
                depths[chunk] = weight_z[:, cut]
                both[chunk, :, :CHUNK] = b_re[:, cut]
                both[chunk, :, CHUNK:] = b_im[:, cut]
                for at, (re, im) in enumerate(((re_high, im_high), (re_low, im_low))):
                    first, second = at * 2 * CHUNK, (at * 2 + 1) * CHUNK
                    right[chunk, :nx, first : first + CHUNK] = re[:, cut]
                    right[chunk, :nx, second : second + CHUNK] = -im[:, cut]
                    right[chunk, nx:, first : first + CHUNK] = im[:, cut]
                    right[chunk, nx:, second : second + CHUNK] = re[:, cut]

        @pl.loop(0, (filled + CHUNK - 1) // CHUNK)
        def _(chunk):
            begin = chunk * CHUNK
            final = jnp.minimum(begin + CHUNK, filled)
            first = sum((end <= begin).astype(jnp.int32) for end in ends[:-1])
            last = sum((end < final).astype(jnp.int32) for end in ends[:-1])
            low_plane = first * (PLANES // BINS)
            for span in range(BINS):

                @pl.when(last - first == span)
                def _(planes=(span + 1) * (PLANES // BINS) + TAPS - 1):
                    here = both[chunk]
                    for z in range(planes):
                        line = depths[chunk, pl.ds(low_plane + z, 1), :]
                        high, low = halves(here * jnp.concatenate([line, line], axis=1))
                        left[z * ny : (z + 1) * ny, : 2 * CHUNK] = high
                        left[z * ny : (z + 1) * ny, 2 * CHUNK :] = low
                    high, low = left[: planes * ny, : 2 * CHUNK], left[: planes * ny, 2 * CHUNK :]
                    right_high, right_low = right[chunk, :, : 2 * CHUNK], right[chunk, :, 2 * CHUNK :]
                    sums = lax.dot_general(
                        jnp.concatenate([high, low, high], axis=1),
                        jnp.concatenate([right_high, right_high, right_low], axis=1),
                        (((1,), (1,)), ((), ())),
                        preferred_element_type=F32,
                    )
                    at = pl.ds(pl.multiple_of((slab * PLANES + low_plane) * ny, ny), planes * ny)
                    grid_re[at, :] += sums[:, :nx]
                    grid_im[at, :] += sums[:, nx:]

    tz = table_z[...]
    depth_all = table_z.shape[1] // 3

    @pl.loop(0, ny // 8)
    def _(block):
        at = pl.ds(pl.multiple_of(block * 8, 8), 8)
        g_re = jnp.swapaxes(grid_re.reshape(depth_all, ny, nx)[:, at, :], 0, 1)
        g_im = jnp.swapaxes(grid_im.reshape(depth_all, ny, nx)[:, at, :], 0, 1)
        done_re, done_im = [], []
        for row in range(8):
            sums = fine_dot(tz, jnp.concatenate([g_re[row], g_im[row]], axis=1))
            done_re.append(sums[:nz, :nx] - sums[nz:, nx:])
            done_im.append(sums[nz:, :nx] + sums[:nz, nx:])
        out[0, :, at, :] = jnp.swapaxes(jnp.stack(done_re), 0, 1)
        out[1, :, at, :] = jnp.swapaxes(jnp.stack(done_im), 0, 1)


def turns(outer, inner, length):
    angle = 2.0 * np.pi * ((outer * inner) % length) / length
    return np.cos(angle), np.sin(angle)


def tables(n_slab, n_pencil, nz):
    ny, nx = NY // n_slab, NX // n_pencil
    near, far = np.arange(2 * LOW), np.arange(NY // LOW) * LOW

    def stacked(count, width, inner, length):
        outer = np.arange(count * width).reshape(count, width, 1)
        return turns(outer, inner, length)

    cy, sy = stacked(n_slab, ny, near, NY)
    tap_y = np.concatenate([cy, sy], axis=1)
    cy, sy = stacked(n_slab, ny, far, NY)
    phase_y = np.concatenate(
        [np.concatenate([cy, -sy], axis=2), np.concatenate([sy, cy], axis=2)], axis=1
    )
    cx, sx = stacked(n_pencil, nx, near, NX)
    tap_x = np.concatenate([cx, sx], axis=1)
    cx, sx = stacked(n_pencil, nx, far, NX)
    phase_x = np.concatenate([cx, sx], axis=1)
    cz, sz = turns(np.arange(nz)[:, None], np.arange(nz + 2 * PLANES)[None, :], nz)
    table_z = np.concatenate([cz, sz], axis=0) / math.sqrt(nz * NY * NX)
    stacks = [stack_left(x.astype(np.float32)) for x in (tap_y, phase_y, tap_x, table_z)]
    exact_right = np.delete(stack_left(phase_x.astype(np.float32)), np.s_[: NY // LOW], axis=-1)
    return stacks[0], stacks[1], stacks[2], exact_right, stacks[3]


def shards(n_slab, n_pencil, sample_tile, sample_cell, sample_frac, sample_value):
    n_src = n_slab * n_pencil
    per = sample_tile.shape[0]
    nz = PLANES * n_slab
    ny, nx = NY // n_slab, NX // n_pencil
    capacity = max(2, 2 * per // n_src)
    room = -(-n_pencil * capacity // 8) * 8
    owner = sample_tile[:, 0]
    base_z = owner // n_pencil * PLANES + sample_cell[0]
    base_y = owner % n_pencil * (NY // n_pencil) + sample_cell[1]
    anchor = jnp.stack([base_z, base_y, sample_cell[2]]).astype(F32)
    mine = jnp.concatenate([anchor, sample_frac, sample_value], axis=0)
    order = jnp.arange(per, dtype=jnp.int32)
    key = base_z * per + order
    rank = jnp.sum((key[None, :] < key[:, None]).astype(jnp.int32), axis=1)
    shuffle = (rank[:, None] == order[None, :]).astype(F32)
    mine = jnp.dot(mine, shuffle, precision=lax.Precision.HIGHEST, preferred_element_type=F32)
    feats = gather_all(n_slab, n_pencil, mine)
    bins = jnp.arange(n_slab * BINS + 1, dtype=jnp.int32) * (PLANES // BINS)
    starts = jnp.sum((feats[:, 0, :].astype(jnp.int32)[:, None, :] < bins[None, :, None]).astype(jnp.int32), axis=2)
    most = n_src * room
    chunks = -(-most // GROUP) * (GROUP // CHUNK)
    vmem = pl.BlockSpec(memory_space=pltpu.VMEM)
    volume = pl.pallas_call(
        functools.partial(kernel, n_src, n_slab, per, room, ny, nz),
        out_shape=jax.ShapeDtypeStruct((2, nz, ny, nx), F32),
        in_specs=[pl.BlockSpec(memory_space=pltpu.SMEM)] + [vmem] * 6,
        out_specs=vmem,
        scratch_shapes=[
            pltpu.VMEM((n_src * per + room, 128), F32),
            pltpu.VMEM((-(-most // GROUP) * GROUP + room, 128), F32),
            pltpu.VMEM(((nz + 2 * PLANES) * ny, nx), F32),
            pltpu.VMEM(((nz + 2 * PLANES) * ny, nx), F32),
            pltpu.VMEM((WINDOW * ny, 4 * CHUNK), BF16),
            pltpu.VMEM((chunks, ny, 2 * CHUNK), F32),
            pltpu.VMEM((chunks, 2 * nx, 4 * CHUNK), BF16),
            pltpu.VMEM((chunks, 2 * PLANES, CHUNK), F32),
        ],
        compiler_params=pltpu.CompilerParams(vmem_limit_bytes=67043328),
        name="volume",
    )(starts, feats, *tables(n_slab, n_pencil, nz))
    return volume


def solution(mesh):
    placed_as = (
        P(("slab", "pencil"), None),
        P(None, ("slab", "pencil")),
        P(None, ("slab", "pencil")),
        P(None, ("slab", "pencil")),
    )
    return jax.shard_map(
        functools.partial(shards, mesh.shape["slab"], mesh.shape["pencil"]),
        mesh=mesh,
        in_specs=placed_as,
        out_specs=P(None, None, "slab", "pencil"),
        check_vma=False,
    )
```

```python
import functools
import math

import jax
import jax.numpy as jnp
import numpy as np
from jax import lax
from jax.experimental import pallas as pl
from jax.experimental.pallas import tpu as pltpu
from jax.sharding import PartitionSpec as P

NY = 512
NX = 512
PLANES = 8
TAPS = 8
WINDOW = PLANES + TAPS - 1
LOW = 16
CHUNK = 128
GROUP = 256
MAIN = 11
BINS = 4
BETA = 18.64
F32 = jnp.float32
BF16 = jnp.bfloat16


def series():
    quarter = BETA * BETA / 4.0
    terms = [1.0]
    for order in range(1, 41):
        terms.append(terms[-1] * quarter / float(order * order))
    total = sum(terms)
    return [term / total for term in terms]


SERIES = series()


def tap_weights(frac, taps):
    gap = (taps - 3.0 - frac) * 0.25
    radicand = jnp.maximum(1.0 - gap * gap, 0.0)
    total = jnp.full(radicand.shape, SERIES[-1], F32)
    for coefficient in SERIES[-2::-1]:
        total = total * radicand + coefficient
    return total


def placed(weights, anchor, rows):
    gap = lax.broadcasted_iota(jnp.int32, (rows, anchor.shape[1]), 0) - anchor
    total = jnp.where(gap == 0, weights[0:1], 0.0)
    for tap in range(1, TAPS):
        total = jnp.where(gap == tap, weights[tap : tap + 1], total)
    return total


def halves(value):
    high = value.astype(BF16)
    return high, (value - high.astype(F32)).astype(BF16)


def stack_left(value):
    high = value.astype(jnp.bfloat16)
    low = (value - high.astype(np.float32)).astype(jnp.bfloat16)
    return np.concatenate([high, high, low], axis=-1)


def fine_dot(left, right):
    high, low = halves(right)
    return jnp.dot(left, jnp.concatenate([high, low, high], axis=0), preferred_element_type=F32)


def gather_kernel(n_slab, n_pencil, mine, out, send_sem, recv_sem, own_sem):
    count = n_slab * n_pencil
    me = lax.axis_index("slab") * n_pencil + lax.axis_index("pencil")

    def name(step):
        target = lax.rem(me + step, count)
        return {"slab": target // n_pencil, "pencil": lax.rem(target, n_pencil)}

    own = pltpu.make_async_copy(mine, out.at[me], own_sem)
    own.start()
    barrier = pltpu.get_barrier_semaphore()

    @pl.loop(1, count)
    def _(step):
        pl.semaphore_signal(barrier, inc=1, device_id=name(step), device_id_type=pl.DeviceIdType.MESH)

    pl.semaphore_wait(barrier, count - 1)

    def send(step, slot):
        return pltpu.make_async_remote_copy(
            src_ref=mine,
            dst_ref=out.at[slot],
            send_sem=send_sem.at[step - 1],
            recv_sem=recv_sem.at[step - 1],
            device_id=name(step),
            device_id_type=pl.DeviceIdType.MESH,
        )

    @pl.loop(1, count)
    def _(step):
        send(step, me).start()

    own.wait()

    @pl.loop(1, count)
    def _(step):
        send(step, lax.rem(me + count - step, count)).wait_recv()

    @pl.loop(1, count)
    def _(step):
        send(step, me).wait_send()


def gather_all(n_slab, n_pencil, mine):
    count = n_slab * n_pencil
    vmem = pl.BlockSpec(memory_space=pltpu.VMEM)
    return pl.pallas_call(
        functools.partial(gather_kernel, n_slab, n_pencil),
        out_shape=jax.ShapeDtypeStruct((count,) + mine.shape, mine.dtype),
        in_specs=[vmem],
        out_specs=vmem,
        scratch_shapes=[
            pltpu.SemaphoreType.DMA((count - 1,)),
            pltpu.SemaphoreType.DMA((count - 1,)),
            pltpu.SemaphoreType.DMA,
        ],
        compiler_params=pltpu.CompilerParams(collective_id=0, has_side_effects=True),
        name="gather_samples",
    )(mine)


def kernel(
    n_src, n_slab, per, room, ny, nz,
    starts, feats, tap_y, phase_y, tap_x, phase_x, table_z, out,
    rows, packed, grid_re, grid_im, left_a, left_b, both, right, depths,
):
    slab_here = lax.axis_index("slab")
    pencil_here = lax.axis_index("pencil")
    nx = out.shape[3]
    short = min(room, 24)
    taps = lax.broadcasted_iota(jnp.int32, (TAPS, per), 0).astype(F32)

    @pl.loop(0, n_src, unroll=2)
    def _(src):
        f = feats[src]
        pieces = [f] + [tap_weights(f[3 + d : 4 + d], taps) for d in range(3)]
        rows[pl.ds(pl.multiple_of(src * per, per), per), 0:32] = jnp.concatenate(pieces, axis=0).T

    grid_re[...] = jnp.zeros_like(grid_re)
    grid_im[...] = jnp.zeros_like(grid_im)
    lanes = lax.broadcasted_iota(jnp.int32, (32, GROUP), 1)
    counter = lax.broadcasted_iota(jnp.int32, (NY // LOW, GROUP), 0)
    ty, hy = tap_y[slab_here], phase_y[slab_here]
    tx, hx = tap_x[pencil_here], phase_x[pencil_here]

    @pl.loop(0, n_slab)
    def _(slab):
        ends = []
        filled = jnp.int32(0)
        for part in range(BINS):

            def pack(quad, filled, part=part):
                at = slab * BINS + part
                picks = [(starts[quad * 4 + k, at], starts[quad * 4 + k, at + 1]) for k in range(4)]
                places = [filled]
                for first, end in picks:
                    places.append(places[-1] + end - first)
                longest = functools.reduce(jnp.maximum, [end - first for first, end in picks])

                def move(size):
                    for (first, _), place in zip(picks, places):
                        packed[pl.ds(place, size), :] = rows[pl.ds(first, size), :]

                if short == room:
                    move(room)
                else:
                    pl.when(longest <= short)(functools.partial(move, short))
                    pl.when(longest > short)(functools.partial(move, room))
                return places[-1]

            filled = lax.fori_loop(0, n_src // 4, pack, filled)
            ends.append(filled)

        @pl.loop(0, (filled + GROUP - 1) // GROUP)
        def _(group):
            base = pl.multiple_of(group * GROUP, GROUP)
            f = packed[pl.ds(base, GROUP), :].T[0:32]
            f = jnp.where(lanes + base < filled, f, 0.0)
            whole = f[0:3].astype(jnp.int32)
            high_y, high_x = whole[1:2] // LOW, whole[2:3] // LOW
            weight_z = placed(f[8:16], whole[0:1] - slab * PLANES, 3 * PLANES)
            place_y = placed(f[16:24], whole[1:2] - high_y * LOW, 2 * LOW)
            place_x = placed(f[24:32], whole[2:3] - high_x * LOW, 2 * LOW)
            hit_y = counter == high_y
            hit_x = (counter == high_x).astype(F32).astype(BF16)
            value_y = jnp.concatenate([jnp.where(hit_y, f[6:7], 0.0), jnp.where(hit_y, f[7:8], 0.0)], axis=0)
            near, far = fine_dot(ty, place_y), fine_dot(hy, value_y)
            b_re = near[:ny] * far[:ny] - near[ny:] * far[ny:]
            b_im = near[:ny] * far[ny:] + near[ny:] * far[:ny]
            near = fine_dot(tx, place_x)
            far = jnp.dot(hx, jnp.concatenate([hit_x, hit_x], axis=0), preferred_element_type=F32)
            c_re = near[:nx] * far[:nx] - near[nx:] * far[nx:]
            c_im = near[:nx] * far[nx:] + near[nx:] * far[:nx]
            re_high, re_low = halves(c_re)
            im_high, im_low = halves(c_im)
            for part in range(GROUP // CHUNK):
                cut = slice(part * CHUNK, (part + 1) * CHUNK)
                chunk = group * (GROUP // CHUNK) + part
                depths[chunk] = weight_z[:, cut]
                both[chunk, :, :CHUNK] = b_re[:, cut]
                both[chunk, :, CHUNK:] = b_im[:, cut]
                for at, (re, im) in enumerate(((re_high, im_high), (re_low, im_low))):
                    first, second = at * 2 * CHUNK, (at * 2 + 1) * CHUNK
                    right[chunk, :nx, first : first + CHUNK] = re[:, cut]
                    right[chunk, :nx, second : second + CHUNK] = -im[:, cut]
                    right[chunk, nx:, first : first + CHUNK] = im[:, cut]
                    right[chunk, nx:, second : second + CHUNK] = re[:, cut]

        def bounds(chunk):
            begin = chunk * CHUNK
            final = jnp.minimum(begin + CHUNK, filled)
            first = sum((end <= begin).astype(jnp.int32) for end in ends[:-1])
            last = sum((end < final).astype(jnp.int32) for end in ends[:-1])
            low_plane = jnp.minimum(first * (PLANES // BINS), WINDOW - MAIN)
            return low_plane, (last + 1) * (PLANES // BINS) + TAPS - 1 > low_plane + MAIN

        def form(left, chunk, low_plane, planes):
            here = both[chunk]
            for z in range(planes):
                line = depths[chunk, pl.ds(low_plane + z, 1), :]
                high, low = halves(here * jnp.concatenate([line, line], axis=1))
                left[z * ny : (z + 1) * ny, : 2 * CHUNK] = high
                left[z * ny : (z + 1) * ny, 2 * CHUNK :] = low

        def multiply(left, chunk, low_plane, planes):
            high, low = left[: planes * ny, : 2 * CHUNK], left[: planes * ny, 2 * CHUNK :]
            right_high, right_low = right[chunk, :, : 2 * CHUNK], right[chunk, :, 2 * CHUNK :]
            sums = lax.dot_general(
                jnp.concatenate([high, low, high], axis=1),
                jnp.concatenate([right_high, right_high, right_low], axis=1),
                (((1,), (1,)), ((), ())),
                preferred_element_type=F32,
            )
            at = pl.ds(pl.multiple_of((slab * PLANES + low_plane) * ny, ny), planes * ny)
            grid_re[at, :] += sums[:, :nx]
            grid_im[at, :] += sums[:, nx:]

        form(left_a, 0, bounds(0)[0], MAIN)

        @pl.loop(0, (filled + GROUP - 1) // GROUP)
        def _(pair):
            one, two = pair * 2, pair * 2 + 1
            low_one, more_one = bounds(one)
            low_two, more_two = bounds(two)
            low_next, _ = bounds(two + 1)
            multiply(left_a, one, low_one, MAIN)
            form(left_b, two, low_two, MAIN)
            multiply(left_b, two, low_two, MAIN)
            form(left_a, two + 1, low_next, MAIN)
            for chunk, low_plane, more in ((one, low_one, more_one), (two, low_two, more_two)):

                @pl.when(more)
                def _(chunk=chunk, low_plane=low_plane):
                    form(left_b, chunk, low_plane + MAIN, WINDOW - MAIN)
                    multiply(left_b, chunk, low_plane + MAIN, WINDOW - MAIN)

    tz = table_z[...]
    depth_all = table_z.shape[1] // 3

    @pl.loop(0, ny // 8)
    def _(block):
        at = pl.ds(pl.multiple_of(block * 8, 8), 8)
        g_re = jnp.swapaxes(grid_re.reshape(depth_all, ny, nx)[:, at, :], 0, 1)
        g_im = jnp.swapaxes(grid_im.reshape(depth_all, ny, nx)[:, at, :], 0, 1)
        done_re, done_im = [], []
        for row in range(8):
            sums = fine_dot(tz, jnp.concatenate([g_re[row], g_im[row]], axis=1))
            done_re.append(sums[:nz, :nx] - sums[nz:, nx:])
            done_im.append(sums[nz:, :nx] + sums[:nz, nx:])
        out[0, :, at, :] = jnp.swapaxes(jnp.stack(done_re), 0, 1)
        out[1, :, at, :] = jnp.swapaxes(jnp.stack(done_im), 0, 1)


def turns(outer, inner, length):
    angle = 2.0 * np.pi * ((outer * inner) % length) / length
    return np.cos(angle), np.sin(angle)


def tables(n_slab, n_pencil, nz):
    ny, nx = NY // n_slab, NX // n_pencil
    near, far = np.arange(2 * LOW), np.arange(NY // LOW) * LOW

    def stacked(count, width, inner, length):
        outer = np.arange(count * width).reshape(count, width, 1)
        return turns(outer, inner, length)

    cy, sy = stacked(n_slab, ny, near, NY)
    tap_y = np.concatenate([cy, sy], axis=1)
    cy, sy = stacked(n_slab, ny, far, NY)
    phase_y = np.concatenate(
        [np.concatenate([cy, -sy], axis=2), np.concatenate([sy, cy], axis=2)], axis=1
    )
    cx, sx = stacked(n_pencil, nx, near, NX)
    tap_x = np.concatenate([cx, sx], axis=1)
    cx, sx = stacked(n_pencil, nx, far, NX)
    phase_x = np.concatenate([cx, sx], axis=1)
    cz, sz = turns(np.arange(nz)[:, None], np.arange(nz + 2 * PLANES)[None, :], nz)
    table_z = np.concatenate([cz, sz], axis=0) / math.sqrt(nz * NY * NX)
    stacks = [stack_left(x.astype(np.float32)) for x in (tap_y, phase_y, tap_x, table_z)]
    exact_right = np.delete(stack_left(phase_x.astype(np.float32)), np.s_[: NY // LOW], axis=-1)
    return stacks[0], stacks[1], stacks[2], exact_right, stacks[3]


def shards(n_slab, n_pencil, sample_tile, sample_cell, sample_frac, sample_value):
    n_src = n_slab * n_pencil
    per = sample_tile.shape[0]
    nz = PLANES * n_slab
    ny, nx = NY // n_slab, NX // n_pencil
    capacity = max(2, 2 * per // n_src)
    room = -(-n_pencil * capacity // 8) * 8
    owner = sample_tile[:, 0]
    base_z = owner // n_pencil * PLANES + sample_cell[0]
    base_y = owner % n_pencil * (NY // n_pencil) + sample_cell[1]
    anchor = jnp.stack([base_z, base_y, sample_cell[2]]).astype(F32)
    mine = jnp.concatenate([anchor, sample_frac, sample_value], axis=0)
    order = jnp.arange(per, dtype=jnp.int32)
    key = base_z * per + order
    rank = jnp.sum((key[None, :] < key[:, None]).astype(jnp.int32), axis=1)
    shuffle = (rank[:, None] == order[None, :]).astype(F32)
    mine = jnp.dot(mine, shuffle, precision=lax.Precision.HIGHEST, preferred_element_type=F32)
    feats = gather_all(n_slab, n_pencil, mine)
    bins = jnp.arange(n_slab * BINS + 1, dtype=jnp.int32) * (PLANES // BINS)
    planes = feats[:, 0, :].astype(jnp.int32)
    starts = jnp.sum((planes[:, None, :] < bins[None, :, None]).astype(jnp.int32), axis=2)
    starts = starts + jnp.arange(n_src, dtype=jnp.int32)[:, None] * per
    most = n_src * room
    chunks = -(-most // GROUP) * (GROUP // CHUNK)
    vmem = pl.BlockSpec(memory_space=pltpu.VMEM)
    volume = pl.pallas_call(
        functools.partial(kernel, n_src, n_slab, per, room, ny, nz),
        out_shape=jax.ShapeDtypeStruct((2, nz, ny, nx), F32),
        in_specs=[pl.BlockSpec(memory_space=pltpu.SMEM)] + [vmem] * 6,
        out_specs=vmem,
        scratch_shapes=[
            pltpu.VMEM((n_src * per + room, 128), F32),
            pltpu.VMEM((-(-most // GROUP) * GROUP + room, 128), F32),
            pltpu.VMEM(((nz + 2 * PLANES) * ny, nx), F32),
            pltpu.VMEM(((nz + 2 * PLANES) * ny, nx), F32),
            pltpu.VMEM((MAIN * ny, 4 * CHUNK), BF16),
            pltpu.VMEM((MAIN * ny, 4 * CHUNK), BF16),
            pltpu.VMEM((chunks + 1, ny, 2 * CHUNK), F32),
            pltpu.VMEM((chunks, 2 * nx, 4 * CHUNK), BF16),
            pltpu.VMEM((chunks + 1, 3 * PLANES, CHUNK), F32),
        ],
        compiler_params=pltpu.CompilerParams(vmem_limit_bytes=67043328),
        name="volume",
    )(starts, feats, *tables(n_slab, n_pencil, nz))
    return volume


def solution(mesh):
    placed_as = (
        P(("slab", "pencil"), None),
        P(None, ("slab", "pencil")),
        P(None, ("slab", "pencil")),
        P(None, ("slab", "pencil")),
    )
    return jax.shard_map(
        functools.partial(shards, mesh.shape["slab"], mesh.shape["pencil"]),
        mesh=mesh,
        in_specs=placed_as,
        out_specs=P(None, None, "slab", "pencil"),
        check_vma=False,
    )
```

```python
import functools
import math

import jax
import jax.numpy as jnp
import numpy as np
from jax import lax
from jax.experimental import pallas as pl
from jax.experimental.pallas import tpu as pltpu
from jax.sharding import PartitionSpec as P

NY = 512
NX = 512
PLANES = 8
TAPS = 8
WINDOW = PLANES + TAPS - 1
LOW = 16
CHUNK = 128
GROUP = 256
MAIN = 11
BINS = 4
BETA = 18.64
F32 = jnp.float32
BF16 = jnp.bfloat16


def series():
    quarter = BETA * BETA / 4.0
    terms = [1.0]
    for order in range(1, 41):
        terms.append(terms[-1] * quarter / float(order * order))
    total = sum(terms)
    return [term / total for term in terms]


SERIES = series()


def tap_weights(frac, taps):
    gap = (taps - 3.0 - frac) * 0.25
    radicand = jnp.maximum(1.0 - gap * gap, 0.0)
    total = jnp.full(radicand.shape, SERIES[-1], F32)
    for coefficient in SERIES[-2::-1]:
        total = total * radicand + coefficient
    return total


def placed(weights, anchor, rows):
    gap = lax.broadcasted_iota(jnp.int32, (rows, anchor.shape[1]), 0) - anchor
    total = jnp.where(gap == 0, weights[0:1], 0.0)
    for tap in range(1, TAPS):
        total = jnp.where(gap == tap, weights[tap : tap + 1], total)
    return total


def halves(value):
    high = value.astype(BF16)
    return high, (value - high.astype(F32)).astype(BF16)


def stack_left(value):
    high = value.astype(jnp.bfloat16)
    low = (value - high.astype(np.float32)).astype(jnp.bfloat16)
    return np.concatenate([high, high, low], axis=-1)


def fine_dot(left, right):
    high, low = halves(right)
    return jnp.dot(left, jnp.concatenate([high, low, high], axis=0), preferred_element_type=F32)


def gather_kernel(n_slab, n_pencil, mine, out, send_sem, recv_sem, own_sem, pair_send, pair_recv):
    half = n_pencil // 2
    count = n_slab * half
    slab, pencil = lax.axis_index("slab"), lax.axis_index("pencil")
    parity = lax.rem(pencil, 2)
    me = slab * half + pencil // 2
    partner = {"slab": slab, "pencil": pencil + 1 - 2 * parity}
    mesh_id = pl.DeviceIdType.MESH

    def name(step):
        target = lax.rem(me + step, count)
        return {"slab": target // half, "pencil": lax.rem(target, half) * 2 + parity}

    own = pltpu.make_async_copy(mine, out.at[parity * count + me], own_sem)
    own.start()
    barrier = pltpu.get_barrier_semaphore()

    @pl.loop(1, count)
    def _(step):
        pl.semaphore_signal(barrier, inc=1, device_id=name(step), device_id_type=mesh_id)

    pl.semaphore_signal(barrier, inc=1, device_id=partner, device_id_type=mesh_id)
    pl.semaphore_wait(barrier, count)

    def send(step, slot):
        return pltpu.make_async_remote_copy(
            src_ref=mine,
            dst_ref=out.at[parity * count + slot],
            send_sem=send_sem.at[step - 1],
            recv_sem=recv_sem.at[step - 1],
            device_id=name(step),
            device_id_type=mesh_id,
        )

    @pl.loop(1, count)
    def _(step):
        send(step, me).start()

    own.wait()

    @pl.loop(1, count)
    def _(step):
        send(step, lax.rem(me + count - step, count)).wait_recv()

    ours = out.at[pl.ds(parity * count, count)]
    across = pltpu.make_async_remote_copy(
        src_ref=ours, dst_ref=ours, send_sem=pair_send, recv_sem=pair_recv, device_id=partner, device_id_type=mesh_id
    )
    across.start()

    @pl.loop(1, count)
    def _(step):
        send(step, me).wait_send()

    across.wait()


def gather_all(n_slab, n_pencil, mine):
    count = n_slab * n_pencil
    vmem = pl.BlockSpec(memory_space=pltpu.VMEM)
    return pl.pallas_call(
        functools.partial(gather_kernel, n_slab, n_pencil),
        out_shape=jax.ShapeDtypeStruct((count,) + mine.shape, mine.dtype),
        in_specs=[vmem],
        out_specs=vmem,
        scratch_shapes=[
            pltpu.SemaphoreType.DMA((count // 2 - 1,)),
            pltpu.SemaphoreType.DMA((count // 2 - 1,)),
            pltpu.SemaphoreType.DMA,
            pltpu.SemaphoreType.DMA,
            pltpu.SemaphoreType.DMA,
        ],
        compiler_params=pltpu.CompilerParams(collective_id=0, has_side_effects=True),
        name="gather_samples",
    )(mine)


def kernel(
    n_src, n_slab, per, room, ny, nz,
    starts, feats, tap_y, phase_y, tap_x, phase_x, table_z, out,
    rows, packed, grid_re, grid_im, left_a, left_b, both, right, depths,
):
    slab_here = lax.axis_index("slab")
    pencil_here = lax.axis_index("pencil")
    nx = out.shape[3]
    short = min(room, 24)
    taps = lax.broadcasted_iota(jnp.int32, (TAPS, per), 0).astype(F32)

    @pl.loop(0, n_src, unroll=2)
    def _(src):
        f = feats[src]
        pieces = [f] + [tap_weights(f[3 + d : 4 + d], taps) for d in range(3)]
        rows[pl.ds(pl.multiple_of(src * per, per), per), 0:32] = jnp.concatenate(pieces, axis=0).T

    grid_re[...] = jnp.zeros_like(grid_re)
    grid_im[...] = jnp.zeros_like(grid_im)
    lanes = lax.broadcasted_iota(jnp.int32, (32, GROUP), 1)
    counter = lax.broadcasted_iota(jnp.int32, (NY // LOW, GROUP), 0)
    ty, hy = tap_y[slab_here], phase_y[slab_here]
    tx, hx = tap_x[pencil_here], phase_x[pencil_here]

    @pl.loop(0, n_slab)
    def _(slab):
        ends = []
        filled = jnp.int32(0)
        for part in range(BINS):

            def pack(quad, filled, part=part):
                at = slab * BINS + part
                picks = [(starts[quad * 4 + k, at], starts[quad * 4 + k, at + 1]) for k in range(4)]
                places = [filled]
                for first, end in picks:
                    places.append(places[-1] + end - first)
                longest = functools.reduce(jnp.maximum, [end - first for first, end in picks])

                def move(size):
                    for (first, _), place in zip(picks, places):
                        packed[pl.ds(place, size), :] = rows[pl.ds(first, size), :]

                if short == room:
                    move(room)
                else:
                    pl.when(longest <= short)(functools.partial(move, short))
                    pl.when(longest > short)(functools.partial(move, room))
                return places[-1]

            filled = lax.fori_loop(0, n_src // 4, pack, filled)
            ends.append(filled)

        @pl.loop(0, (filled + GROUP - 1) // GROUP)
        def _(group):
            base = pl.multiple_of(group * GROUP, GROUP)
            f = packed[pl.ds(base, GROUP), :].T[0:32]
            f = jnp.where(lanes + base < filled, f, 0.0)
            whole = f[0:3].astype(jnp.int32)
            high_y, high_x = whole[1:2] // LOW, whole[2:3] // LOW
            weight_z = placed(f[8:16], whole[0:1] - slab * PLANES, 3 * PLANES)
            place_y = placed(f[16:24], whole[1:2] - high_y * LOW, 2 * LOW)
            place_x = placed(f[24:32], whole[2:3] - high_x * LOW, 2 * LOW)
            hit_y = counter == high_y
            hit_x = (counter == high_x).astype(F32).astype(BF16)
            value_y = jnp.concatenate([jnp.where(hit_y, f[6:7], 0.0), jnp.where(hit_y, f[7:8], 0.0)], axis=0)
            near, far = fine_dot(ty, place_y), fine_dot(hy, value_y)
            b_re = near[:ny] * far[:ny] - near[ny:] * far[ny:]
            b_im = near[:ny] * far[ny:] + near[ny:] * far[:ny]
            near = fine_dot(tx, place_x)
            far = jnp.dot(hx, jnp.concatenate([hit_x, hit_x], axis=0), preferred_element_type=F32)
            c_re = near[:nx] * far[:nx] - near[nx:] * far[nx:]
            c_im = near[:nx] * far[nx:] + near[nx:] * far[:nx]
            re_high, re_low = halves(c_re)
            im_high, im_low = halves(c_im)
            for part in range(GROUP // CHUNK):
                cut = slice(part * CHUNK, (part + 1) * CHUNK)
                chunk = group * (GROUP // CHUNK) + part
                depths[chunk] = weight_z[:, cut]
                both[chunk, :, :CHUNK] = b_re[:, cut]
                both[chunk, :, CHUNK:] = b_im[:, cut]
                for at, (re, im) in enumerate(((re_high, im_high), (re_low, im_low))):
                    first, second = at * 2 * CHUNK, (at * 2 + 1) * CHUNK
                    right[chunk, :nx, first : first + CHUNK] = re[:, cut]
                    right[chunk, :nx, second : second + CHUNK] = -im[:, cut]
                    right[chunk, nx:, first : first + CHUNK] = im[:, cut]
                    right[chunk, nx:, second : second + CHUNK] = re[:, cut]

        def bounds(chunk):
            begin = chunk * CHUNK
            final = jnp.minimum(begin + CHUNK, filled)
            first = sum((end <= begin).astype(jnp.int32) for end in ends[:-1])
            last = sum((end < final).astype(jnp.int32) for end in ends[:-1])
            low_plane = jnp.minimum(first * (PLANES // BINS), WINDOW - MAIN)
            return low_plane, (last + 1) * (PLANES // BINS) + TAPS - 1 > low_plane + MAIN

        def form(left, chunk, low_plane, planes):
            here = both[chunk]
            for z in range(planes):
                line = depths[chunk, pl.ds(low_plane + z, 1), :]
                high, low = halves(here * jnp.concatenate([line, line], axis=1))
                left[z * ny : (z + 1) * ny, : 2 * CHUNK] = high
                left[z * ny : (z + 1) * ny, 2 * CHUNK :] = low

        def multiply(left, chunk, low_plane, planes):
            high, low = left[: planes * ny, : 2 * CHUNK], left[: planes * ny, 2 * CHUNK :]
            right_high, right_low = right[chunk, :, : 2 * CHUNK], right[chunk, :, 2 * CHUNK :]
            sums = lax.dot_general(
                jnp.concatenate([high, low, high], axis=1),
                jnp.concatenate([right_high, right_high, right_low], axis=1),
                (((1,), (1,)), ((), ())),
                preferred_element_type=F32,
            )
            at = pl.ds(pl.multiple_of((slab * PLANES + low_plane) * ny, ny), planes * ny)
            grid_re[at, :] += sums[:, :nx]
            grid_im[at, :] += sums[:, nx:]

        form(left_a, 0, bounds(0)[0], MAIN)

        @pl.loop(0, (filled + GROUP - 1) // GROUP)
        def _(pair):
            one, two = pair * 2, pair * 2 + 1
            low_one, more_one = bounds(one)
            low_two, more_two = bounds(two)
            low_next, _ = bounds(two + 1)
            multiply(left_a, one, low_one, MAIN)
            form(left_b, two, low_two, MAIN)
            multiply(left_b, two, low_two, MAIN)
            form(left_a, two + 1, low_next, MAIN)
            for chunk, low_plane, more in ((one, low_one, more_one), (two, low_two, more_two)):

                @pl.when(more)
                def _(chunk=chunk, low_plane=low_plane):
                    form(left_b, chunk, low_plane + MAIN, WINDOW - MAIN)
                    multiply(left_b, chunk, low_plane + MAIN, WINDOW - MAIN)

    tz = table_z[...]
    depth_all = table_z.shape[1] // 3

    @pl.loop(0, ny // 8)
    def _(block):
        at = pl.ds(pl.multiple_of(block * 8, 8), 8)
        g_re = jnp.swapaxes(grid_re.reshape(depth_all, ny, nx)[:, at, :], 0, 1)
        g_im = jnp.swapaxes(grid_im.reshape(depth_all, ny, nx)[:, at, :], 0, 1)
        done_re, done_im = [], []
        for row in range(8):
            sums = fine_dot(tz, jnp.concatenate([g_re[row], g_im[row]], axis=1))
            done_re.append(sums[:nz, :nx] - sums[nz:, nx:])
            done_im.append(sums[nz:, :nx] + sums[:nz, nx:])
        out[0, :, at, :] = jnp.swapaxes(jnp.stack(done_re), 0, 1)
        out[1, :, at, :] = jnp.swapaxes(jnp.stack(done_im), 0, 1)


def turns(outer, inner, length):
    angle = 2.0 * np.pi * ((outer * inner) % length) / length
    return np.cos(angle), np.sin(angle)


def tables(n_slab, n_pencil, nz):
    ny, nx = NY // n_slab, NX // n_pencil
    near, far = np.arange(2 * LOW), np.arange(NY // LOW) * LOW

    def stacked(count, width, inner, length):
        outer = np.arange(count * width).reshape(count, width, 1)
        return turns(outer, inner, length)

    cy, sy = stacked(n_slab, ny, near, NY)
    tap_y = np.concatenate([cy, sy], axis=1)
    cy, sy = stacked(n_slab, ny, far, NY)
    phase_y = np.concatenate(
        [np.concatenate([cy, -sy], axis=2), np.concatenate([sy, cy], axis=2)], axis=1
    )
    cx, sx = stacked(n_pencil, nx, near, NX)
    tap_x = np.concatenate([cx, sx], axis=1)
    cx, sx = stacked(n_pencil, nx, far, NX)
    phase_x = np.concatenate([cx, sx], axis=1)
    cz, sz = turns(np.arange(nz)[:, None], np.arange(nz + 2 * PLANES)[None, :], nz)
    table_z = np.concatenate([cz, sz], axis=0) / math.sqrt(nz * NY * NX)
    stacks = [stack_left(x.astype(np.float32)) for x in (tap_y, phase_y, tap_x, table_z)]
    exact_right = np.delete(stack_left(phase_x.astype(np.float32)), np.s_[: NY // LOW], axis=-1)
    return stacks[0], stacks[1], stacks[2], exact_right, stacks[3]


def shards(n_slab, n_pencil, sample_tile, sample_cell, sample_frac, sample_value):
    n_src = n_slab * n_pencil
    per = sample_tile.shape[0]
    nz = PLANES * n_slab
    ny, nx = NY // n_slab, NX // n_pencil
    capacity = max(2, 2 * per // n_src)
    room = -(-n_pencil * capacity // 8) * 8
    owner = sample_tile[:, 0]
    base_z = owner // n_pencil * PLANES + sample_cell[0]
    base_y = owner % n_pencil * (NY // n_pencil) + sample_cell[1]
    anchor = jnp.stack([base_z, base_y, sample_cell[2]]).astype(F32)
    mine = jnp.concatenate([anchor, sample_frac, sample_value], axis=0)
    order = jnp.arange(per, dtype=jnp.int32)
    key = base_z * per + order
    rank = jnp.sum((key[None, :] < key[:, None]).astype(jnp.int32), axis=1)
    shuffle = (rank[:, None] == order[None, :]).astype(F32)
    mine = jnp.dot(mine, shuffle, precision=lax.Precision.HIGHEST, preferred_element_type=F32)
    feats = gather_all(n_slab, n_pencil, mine)
    bins = jnp.arange(n_slab * BINS + 1, dtype=jnp.int32) * (PLANES // BINS)
    planes = feats[:, 0, :].astype(jnp.int32)
    starts = jnp.sum((planes[:, None, :] < bins[None, :, None]).astype(jnp.int32), axis=2)
    starts = starts + jnp.arange(n_src, dtype=jnp.int32)[:, None] * per
    most = n_src * room
    chunks = -(-most // GROUP) * (GROUP // CHUNK)
    vmem = pl.BlockSpec(memory_space=pltpu.VMEM)
    volume = pl.pallas_call(
        functools.partial(kernel, n_src, n_slab, per, room, ny, nz),
        out_shape=jax.ShapeDtypeStruct((2, nz, ny, nx), F32),
        in_specs=[pl.BlockSpec(memory_space=pltpu.SMEM)] + [vmem] * 6,
        out_specs=vmem,
        scratch_shapes=[
            pltpu.VMEM((n_src * per + room, 128), F32),
            pltpu.VMEM((-(-most // GROUP) * GROUP + room, 128), F32),
            pltpu.VMEM(((nz + 2 * PLANES) * ny, nx), F32),
            pltpu.VMEM(((nz + 2 * PLANES) * ny, nx), F32),
            pltpu.VMEM((MAIN * ny, 4 * CHUNK), BF16),
            pltpu.VMEM((MAIN * ny, 4 * CHUNK), BF16),
            pltpu.VMEM((chunks + 1, ny, 2 * CHUNK), F32),
            pltpu.VMEM((chunks, 2 * nx, 4 * CHUNK), BF16),
            pltpu.VMEM((chunks + 1, 3 * PLANES, CHUNK), F32),
        ],
        compiler_params=pltpu.CompilerParams(vmem_limit_bytes=67043328),
        name="volume",
    )(starts, feats, *tables(n_slab, n_pencil, nz))
    return volume


def solution(mesh):
    placed_as = (
        P(("slab", "pencil"), None),
        P(None, ("slab", "pencil")),
        P(None, ("slab", "pencil")),
        P(None, ("slab", "pencil")),
    )
    return jax.shard_map(
        functools.partial(shards, mesh.shape["slab"], mesh.shape["pencil"]),
        mesh=mesh,
        in_specs=placed_as,
        out_specs=P(None, None, "slab", "pencil"),
        check_vma=False,
    )
```
